128 devices in a mesh: row: 8 (over z, core), col: 16 (over y, x).
Axes of the slice: x: 4, y: 4, z: 4, core: 2. Of those that a mesh axis runs over, the one named last changes fastest.
Arguments:
- a_matrix: bfloat16 [16384, 16384], P('row', 'col'), may hold values from -6 to 6
- a_flags: int32 [128, 128], P('row', 'col'), may hold values from 0 to 1, as said below
- b_matrix: bfloat16 [16384, 32768], P('row', 'col'), may hold values from -0.1875 to 0.1875
- b_flags: int32 [128, 256], P('row', 'col'), may hold values from 0 to 1, as said below
- sections: int32 [2], replicated, may hold values from 0 to 15
Outputs:
- packed: bfloat16 [16384, 32768], P('row', 'col')
- tile_place: int32 [128, 256], P('row', 'col')
The draws below stay inside these ranges and needn't reach their ends.
Inputs may be any that keep to these rules, and one draw needn't show every extreme that they name: `a_flags`: 0 or 1; the 16 x 8 tiles of one device hold at most 64 ones, and some device holds exactly 64. `b_flags`: 0 or 1; each aligned block of 8 x 16 tiles holds at most 64 ones, and some block exactly 64.
All inputs are finite; a program needn't handle non-finite values.
Results may differ from the reference program's by a relative error of at most 0.001.
Values may be sent and summed in bfloat16 or wider, within the bound.
A program may use at most 128 MiB of HBM per device.

```python
import jax
import jax.numpy as jnp
from jax import lax

TILE = 128
TM_DEV = 16
TN_DEV = 16
KT = 8
SECTIONS = 2
MOST = 64
N_ROW = 8
N_COL = 16


def block_flags(key, row_blocks, col_blocks, block_rows, block_cols, ceiling):
    number = row_blocks * col_blocks
    per_block = block_rows * block_cols
    first, second, third = jax.random.split(key, 3)
    counts = jax.random.randint(first, (number,), max(1, ceiling // 4), ceiling + 1)
    chosen = jax.random.randint(second, (), 0, number)
    counts = jnp.where(jnp.arange(number) == chosen, ceiling, counts)
    scores = jax.random.randint(third, (number, per_block), 0, 1 << 20) * per_block + jnp.arange(per_block)[None, :]
    order = jnp.argsort(scores, axis=1, stable=True)
    ranking = jnp.argsort(order, axis=1, stable=True)
    flags = (ranking < counts[:, None]).astype(jnp.int32)
    flags = flags.reshape(row_blocks, col_blocks, block_rows, block_cols).transpose(0, 2, 1, 3)
    return flags.reshape(row_blocks * block_rows, col_blocks * block_cols)


def draw_a_flags(key, part):
    return block_flags(jax.random.fold_in(key, 11), N_ROW, N_COL, TM_DEV, KT, MOST)


def draw_b_flags(key, part):
    return block_flags(jax.random.fold_in(key, 23), N_COL, N_COL, KT, TN_DEV, MOST)


def steps_of(own_key, shape, cuts, smallest, largest):
    factor_of, own = 1.0, jax.random.fold_in(own_key, 6)
    for dim, shards_of in cuts:
        heights = jnp.exp(jax.random.uniform(jax.random.fold_in(own, dim), (shards_of,), jnp.float32, smallest / len(cuts), largest / len(cuts)))
        factor_of = factor_of * jnp.repeat(heights, shape[dim] // shards_of).reshape([-1 if axis == dim else 1 for axis in range(len(shape))])
    return factor_of


def centred(own_key, shape, width, limit, cuts=(), held_as=jnp.bfloat16):
    drawn = width * jax.random.normal(own_key, shape, jnp.float32)
    if cuts:
        drawn = drawn * steps_of(own_key, shape, cuts, -0.22, 0.18)
    return jnp.clip(drawn, -limit, limit).astype(held_as)


def setup_inputs(seed: int = 0) -> dict:
    keys = jax.random.split(jax.random.key(seed), 6)
    a_matrix = centred(keys[0], (TILE * TM_DEV * N_ROW, TILE * KT * N_COL), 1.0, 6.0, ((0, 8), (1, 16)))
    a_flags = draw_a_flags(jax.random.fold_in(keys[5], 71), 0)
    b_matrix = centred(keys[2], (TILE * KT * N_COL, TILE * TN_DEV * N_COL), (KT * TILE) ** -0.5, 0.1875, ((0, 8), (1, 16)))
    b_flags = draw_b_flags(jax.random.fold_in(keys[5], 71), 0)
    sections = jax.random.randint(keys[4], (SECTIONS,), 0, N_COL).astype(jnp.int32)
    return {"a_matrix": a_matrix, "a_flags": a_flags, "b_matrix": b_matrix, "b_flags": b_flags, "sections": sections}


def mask_tiles(matrix, flags, tile_rows, tile_cols):
    shaped = matrix.reshape(tile_rows, TILE, tile_cols, TILE)
    shaped = shaped * flags.astype(matrix.dtype)[:, None, :, None]
    return shaped.reshape(tile_rows * TILE, tile_cols * TILE)


def to_tiles(matrix, tile_rows, tile_cols):
    return matrix.reshape(tile_rows, TILE, tile_cols, TILE).transpose(0, 2, 1, 3).reshape(tile_rows * tile_cols, TILE, TILE)


def from_tiles(tiles, tile_rows, tile_cols):
    return tiles.reshape(tile_rows, tile_cols, TILE, TILE).transpose(0, 2, 1, 3).reshape(tile_rows * TILE, tile_cols * TILE)


def compact(tiles, flags_flat, capacity):
    rank_of = jnp.cumsum(flags_flat) - 1
    slot_ids = jnp.arange(capacity, dtype=jnp.int32)
    matched = (flags_flat[None, :] == 1) & (rank_of[None, :] == slot_ids[:, None])
    source = jnp.sum(jnp.where(matched, jnp.arange(flags_flat.shape[0], dtype=jnp.int32)[None, :], 0), axis=1).astype(jnp.int32)
    is_valid = jnp.any(matched, axis=1)
    return jnp.take(tiles, source, axis=0) * is_valid.astype(tiles.dtype)[:, None, None]


def reference(a_matrix, a_flags, b_matrix, b_flags, sections):
    panel_width = KT * TILE

    def one_block(block):
        row_index = (block // N_COL).astype(jnp.int32)
        col_index = (block % N_COL).astype(jnp.int32)
        product = jnp.zeros((TM_DEV * TILE, TN_DEV * TILE), jnp.float32)
        intersection = jnp.zeros((TM_DEV, TN_DEV), jnp.float32)
        for step_index in range(SECTIONS):
            section = sections[step_index].astype(jnp.int32)
            a_panel = lax.dynamic_slice(a_matrix, (row_index * TM_DEV * TILE, section * panel_width), (TM_DEV * TILE, panel_width))
            a_panel_flags = lax.dynamic_slice(a_flags, (row_index * TM_DEV, section * KT), (TM_DEV, KT))
            b_panel = lax.dynamic_slice(b_matrix, (section * panel_width, col_index * TN_DEV * TILE), (panel_width, TN_DEV * TILE))
            b_panel_flags = lax.dynamic_slice(b_flags, (section * KT, col_index * TN_DEV), (KT, TN_DEV))
            a_masked = mask_tiles(a_panel, a_panel_flags, TM_DEV, KT)
            b_masked = mask_tiles(b_panel, b_panel_flags, KT, TN_DEV)
            product = product + jnp.dot(a_masked.astype(jnp.float32), b_masked.astype(jnp.float32), precision=lax.Precision.HIGHEST)
            intersection = intersection + jnp.dot(a_panel_flags.astype(jnp.float32), b_panel_flags.astype(jnp.float32), precision=lax.Precision.HIGHEST)
        occupied = (intersection > 0.5).astype(jnp.int32).reshape(-1)
        tiles = to_tiles(product.astype(jnp.bfloat16), TM_DEV, TN_DEV)
        packed_block = from_tiles(compact(tiles, occupied, TM_DEV * TN_DEV), TM_DEV, TN_DEV)
        return packed_block, jnp.sum(occupied).astype(jnp.int32)

    blocks, filled = lax.map(one_block, jnp.arange(N_ROW * N_COL, dtype=jnp.int32))
    offset = (jnp.cumsum(filled) - filled).astype(jnp.int32)
    slot_ids = jnp.arange(TM_DEV * TN_DEV, dtype=jnp.int32)
    places = jnp.where(slot_ids[None, :] < filled[:, None], offset[:, None] + slot_ids[None, :], -1).astype(jnp.int32)
    tile_place = places.reshape(N_ROW, N_COL, TM_DEV, TN_DEV).transpose(0, 2, 1, 3).reshape(N_ROW * TM_DEV, N_COL * TN_DEV)
    packed = blocks.reshape(N_ROW, N_COL, TM_DEV * TILE, TN_DEV * TILE).transpose(0, 2, 1, 3).reshape(N_ROW * TM_DEV * TILE, N_COL * TN_DEV * TILE)
    return packed, tile_place
```

```python
import jax
import jax.numpy as jnp
from jax import lax
from jax.experimental import pallas as pl
from jax.experimental.pallas import tpu as pltpu
from jax.sharding import PartitionSpec as P

TILE = 128
KT = 8
MOST = 64
N_ROW = 8
N_COL = 16
B_LANE = 16
MESH = pl.DeviceIdType.MESH
VMEM = pl.BlockSpec(memory_space=pltpu.VMEM)
SMEM = pl.BlockSpec(memory_space=pltpu.SMEM)
ANY = pl.BlockSpec(memory_space=pl.ANY)


def tiles_of(*lead):
    return (*lead, TILE, TILE)


def pack_kernel(sec, af, bf, af_v, bf_v, a_hbm, b_hbm, pa, pb, msg, src_a, src_b0, src_b1, sems):
    def listed(flag_at, count, src):
        def step(i, found):
            src[found] = i
            return found + flag_at(i)

        return lax.fori_loop(0, count, step, jnp.int32(0), unroll=8)

    def copy_of(matrix, row, col, dst, sem):
        return pltpu.make_async_copy(
            matrix.at[pl.ds(pl.multiple_of(row * TILE, TILE), TILE), pl.ds(pl.multiple_of(col * TILE, TILE), TILE)],
            dst,
            sem,
        )

    def start_a():
        found = listed(lambda i: af[i // KT, i % KT], 16 * KT, src_a)

        def go(j, _):
            i = jnp.where(j < found, src_a[j], 0)
            copy_of(a_hbm, i // KT, i % KT, pa.at[j], sems.at[0]).start()
            return 0

        lax.fori_loop(0, MOST, go, 0, unroll=4)

    def start_b(s, src):
        first = (sec[s] % 2) * KT
        found = listed(lambda i: bf[first + i // 16, i % 16], 16 * KT, src)

        def go(j, _):
            i = jnp.where(j < found, src[j], 0)
            copy_of(b_hbm, first + i // 16, i % 16, pb.at[s, j], sems.at[1 + s]).start()
            return 0

        lax.fori_loop(0, MOST, go, 0, unroll=4)

    start_b(0, src_b0)
    start_b(1, src_b1)
    start_a()
    msg[...] = jnp.zeros_like(msg)
    msg[:, 0:KT] = af_v[...]
    msg[:, B_LANE : B_LANE + 16] = bf_v[...]
    pltpu.make_async_copy(pb.at[0], pb.at[0], sems.at[1]).wait()
    pltpu.make_async_copy(pb.at[1], pb.at[1], sems.at[2]).wait()
    pltpu.make_async_copy(pa, pa, sems.at[0]).wait()


def packed_panels(sections, a_flags, b_flags, a_matrix, b_matrix):
    return pl.pallas_call(
        pack_kernel,
        out_shape=(
            jax.ShapeDtypeStruct(tiles_of(MOST), jnp.bfloat16),
            jax.ShapeDtypeStruct(tiles_of(2, MOST), jnp.bfloat16),
            jax.ShapeDtypeStruct((16, 128), jnp.int32),
        ),
        in_specs=[SMEM, SMEM, SMEM, VMEM, VMEM, ANY, ANY],
        out_specs=(VMEM, VMEM, VMEM),
        scratch_shapes=[
            pltpu.SMEM((136,), jnp.int32),
            pltpu.SMEM((136,), jnp.int32),
            pltpu.SMEM((136,), jnp.int32),
            pltpu.SemaphoreType.DMA((3,)),
        ],
        compiler_params=pltpu.CompilerParams(vmem_limit_bytes=24 << 20),
        name="pack",
    )(sections, a_flags, b_flags, a_flags, b_flags, a_matrix, b_matrix)


N_SEMS = 160


def exchange_kernel(
    sec, pa, pb, msg,
    af, bf, afl, bfl, off,
    cand_0, cand_1, trans, pick, cand2_0, cand2_1, trans2,
    x_buf, y_buf, z_tr, z_dir, z_mg, z_send,
    f_a, f_b, c_a, c_b, cnt, tot,
    send_sems, recv_sems,
):
    cand, cand2 = (cand_0, cand_1), (cand2_0, cand2_1)
    r, c = lax.axis_index("row"), lax.axis_index("col")
    z, core = r // 2, r % 2
    y, x = c // 4, c % 4
    pos = {"x": x, "y": y, "z": z}

    def at(dim, step):
        where = dict(pos)
        where[dim] = (pos[dim] + step) % 4
        return (where["z"] * 2 + core, where["y"] * 4 + where["x"])

    partner = (z * 2 + 1 - core, c)
    col_peers = [(r, (c + d) % N_COL) for d in range(1, N_COL)]
    row_peers = [((r + d) % N_ROW, c) for d in range(1, N_ROW)]

    barrier = pltpu.get_barrier_semaphore()
    for peer in col_peers + row_peers:
        pl.semaphore_signal(barrier, inc=1, device_id=peer, device_id_type=MESH)
    pl.semaphore_wait(barrier, len(col_peers) + len(row_peers))

    started = []

    def send(src, dst, peer):
        n = len(started)
        copy = pltpu.make_async_remote_copy(
            src_ref=src, dst_ref=dst, send_sem=send_sems.at[n], recv_sem=recv_sems.at[n],
            device_id=peer, device_id_type=MESH,
        )
        copy.start()
        started.append(copy)
        return copy

    sec_v = [sec[0], sec[1]]
    root = [{"x": lax.rem(v, 4), "y": lax.div(v, 4), "z": lax.div(v, 4)} for v in sec_v]
    root_core = [lax.rem(lax.div(v, 2), 2) for v in sec_v]

    flags_row = [send(msg, f_a.at[c], peer) for peer in col_peers]
    flags_col = [send(msg, f_b.at[r], peer) for peer in row_peers]

    axes = (("x", "y"), ("y", "x"))
    a1 = []
    for h in range(2):
        d, p = axes[h][0], pos[axes[h][0]]
        far = h * 32 + ((p + 2) % 4) * 8
        a1.append([
            send(pa.at[pl.ds(far, 4)], trans.at[h, 0], at(d, 1)),
            send(pa.at[pl.ds(far + 4, 4)], trans.at[h, 1], at(d, 3)),
        ])
    b0 = [send(pb.at[s, pl.ds((1 - core) * 32, 32)], x_buf.at[s, core], partner) for s in range(2)]
    for h in range(2):
        d, p = axes[h][0], pos[axes[h][0]]
        a1[h] += [
            send(pa.at[pl.ds(h * 32 + ((p + 1) % 4) * 8, 8)], cand[h].at[p], at(d, 1)),
            send(pa.at[pl.ds(h * 32 + ((p + 3) % 4) * 8, 8)], cand[h].at[p], at(d, 3)),
        ]
    f_a[c] = msg[...]
    f_b[r] = msg[...]
    for s in range(2):
        x_buf[s, core] = pb[s, pl.ds(core * 32, 32)]
    for h in range(2):
        p = pos[axes[h][0]]
        cand[h][p] = pa[pl.ds(h * 32 + p * 8, 8)]

    for copy in flags_row + flags_col:
        copy.wait_recv()
    inter = jnp.zeros((16, 128), jnp.int32)
    for s in range(2):
        a_own = f_a[sec_v[s]]
        b_pair = f_b[lax.div(sec_v[s], 2)]
        b_own = jnp.where(lax.rem(sec_v[s], 2) == 0, b_pair[0:KT], b_pair[KT:])
        afl[s] = a_own
        bfl[s] = b_own
        for k in range(KT):
            inter = inter + a_own[:, k : k + 1] * b_own[k : k + 1, :]
    lane = lax.broadcasted_iota(jnp.int32, (16, 128), 1)
    held = (inter > 0) & (lane >= B_LANE) & (lane < B_LANE + 16)
    filled = jnp.sum(jnp.where(held, 1, 0), axis=(0, 1), keepdims=True)
    cnt[...] = jnp.broadcast_to(filled, (8, 128))
    counts = [send(cnt, c_a.at[c], peer) for peer in col_peers]
    c_a[c] = cnt[...]

    for copy in b0:
        copy.wait_recv()
    for s in range(2):
        for i in range(8):
            y_buf[i, s] = x_buf[s, root_core[s], i * 4 : i * 4 + 4]
    w = z
    b1 = [
        send(y_buf.at[((w + 2) % 4) * 2], z_tr.at[0], at("z", 1)),
        send(y_buf.at[((w + 2) % 4) * 2 + 1], z_tr.at[1], at("z", 3)),
        send(y_buf.at[((w + 1) % 4) * 2 + 1], z_dir.at[1], at("z", 1)),
        send(y_buf.at[((w + 3) % 4) * 2], z_dir.at[0], at("z", 3)),
    ]

    for h in range(2):
        d, p = axes[h][0], pos[axes[h][0]]
        a1[h][0].wait_recv()
        a1[h].append(send(trans.at[h, 0], cand[h].at[(p + 3) % 4, pl.ds(0, 4)], at(d, 1)))
        a1[h][1].wait_recv()
        a1[h].append(send(trans.at[h, 1], cand[h].at[(p + 1) % 4, pl.ds(4, 4)], at(d, 3)))

    for copy in counts:
        copy.wait_recv()
    place = lax.broadcasted_iota(jnp.int32, (N_COL, 8, 128), 0)
    all_counts = c_a[...]
    within = jnp.sum(jnp.where(place < c, all_counts, 0), axis=0)
    tot[...] = jnp.sum(all_counts, axis=0)
    totals = [send(tot, c_b.at[r], peer) for peer in row_peers]
    c_b[r] = tot[...]

    a2 = []
    for h in range(2):
        for n in (2, 3, 4, 5):
            a1[h][n].wait_recv()
        d, q = axes[h][1], pos[axes[h][1]]
        for s in range(2):
            for j in range(8):
                pick[h, j, s] = cand[h][root[s][axes[h][0]], j]
        far = ((q + 2) % 4) * 2
        a2.append([
            send(pick.at[h, far], trans2.at[h, 0], at(d, 1)),
            send(pick.at[h, far + 1], trans2.at[h, 1], at(d, 3)),
            send(pick.at[h, pl.ds(((q + 1) % 4) * 2, 2)], cand2[h].at[q], at(d, 1)),
            send(pick.at[h, pl.ds(((q + 3) % 4) * 2, 2)], cand2[h].at[q], at(d, 3)),
        ])
        cand2[h][q] = pick[h, pl.ds(q * 2, 2)]

    def z_merged(t, own_at):
        for s in range(2):
            here = root[s]["z"] == w
            z_send[t, s] = jnp.where(here, y_buf[own_at, s], z_tr[t, s])

    b1[0].wait_recv()
    z_merged(0, ((w + 1) % 4) * 2)
    b1.append(send(z_send.at[0], z_mg.at[0], at("z", 1)))
    b1[1].wait_recv()
    z_merged(1, ((w + 3) % 4) * 2 + 1)
    b1.append(send(z_send.at[1], z_mg.at[1], at("z", 3)))

    for h in range(2):
        d, q = axes[h][1], pos[axes[h][1]]
        a2[h][0].wait_recv()
        a2[h].append(send(trans2.at[h, 0], cand2[h].at[(q + 3) % 4, 0], at(d, 1)))
        a2[h][1].wait_recv()
        a2[h].append(send(trans2.at[h, 1], cand2[h].at[(q + 1) % 4, 1], at(d, 3)))

    def a_slot(h, p, q):
        return h * 32 + p * 8 + q * 2

    a3 = []
    for h in range(2):
        for n in (2, 3, 4, 5):
            a2[h][n].wait_recv()
        p, (d, q) = pos[axes[h][0]], (axes[h][1], pos[axes[h][1]])
        own = a_slot(h, p, q)
        for s in range(2):
            for t in range(2):
                af[own + t, s] = cand2[h][root[s][d], t, s]
        block = af.at[pl.ds(own, 2)]
        a3.append([send(block, block, at(d, 1)), send(block, block, at(d, 3))])

    a4 = []

    def a_out(h, e):
        d, p = axes[h][0], pos[axes[h][0]]
        q = (pos[axes[h][1]] - e) % 4
        block = af.at[pl.ds(a_slot(h, p, q), 2)]
        a4.append((h, q, send(block, block, at(d, 1)), send(block, block, at(d, 3))))

    for h in range(2):
        a_out(h, 0)
    for h in range(2):
        d, p, q = axes[h][1], pos[axes[h][0]], pos[axes[h][1]]
        a3[h][0].wait_recv()
        part = af.at[a_slot(h, p, (q + 3) % 4)]
        a3[h].append(send(part, part, at(d, 1)))
        a3[h][1].wait_recv()
        part = af.at[a_slot(h, p, (q + 1) % 4) + 1]
        a3[h].append(send(part, part, at(d, 3)))
    for e in (1, 3):
        for h in range(2):
            a_out(h, e)

    b1[4].wait_recv()
    b1[5].wait_recv()
    b1[2].wait_recv()
    b1[3].wait_recv()
    mine = core * 8 + w * 2
    for t in range(2):
        for s in range(2):
            ahead = lax.rem(root[s]["z"] - w + 4, 4)
            near = 1 if t == 0 else 3
            got = jnp.where(ahead == near, z_dir[t, s], z_mg[t, s])
            bf[mine + t, s] = jnp.where(ahead == 0, y_buf[w * 2 + t, s], got)

    b2 = {}
    b3 = []

    def b_part(step, t):
        return bf.at[core * 8 + ((w + step) % 4) * 2 + t]

    for t in range(2):
        ref = b_part(0, t)
        b2["up", t] = send(ref, ref, at("z", 1))
        ref = b_part(0, 1 - t)
        b2["down", 1 - t] = send(ref, ref, at("z", 3))
    for t in range(2):
        ref = b_part(0, t)
        b3.append(send(ref, ref, partner))

    for h in range(2):
        a3[h][2].wait_recv()
        a3[h][3].wait_recv()
        a_out(h, 2)

    a5 = []

    def a_forward(n):
        h, q, up, down = a4[n]
        d, p = axes[h][0], pos[axes[h][0]]
        up.wait_recv()
        part = af.at[a_slot(h, (p + 3) % 4, q)]
        a5.append(send(part, part, at(d, 1)))
        down.wait_recv()
        part = af.at[a_slot(h, (p + 1) % 4, q) + 1]
        a5.append(send(part, part, at(d, 3)))

    for n in range(4):
        a_forward(n)
    b2["up", 0].wait_recv()
    ref = b_part(3, 0)
    b2["up", 2] = send(ref, ref, at("z", 1))
    b3.append(send(ref, ref, partner))
    b2["down", 1].wait_recv()
    ref = b_part(1, 1)
    b2["down", 2] = send(ref, ref, at("z", 3))
    b3.append(send(ref, ref, partner))
    for n in range(4, 8):
        a_forward(n)
    for key, step, t in ((("up", 1), 3, 1), (("down", 0), 1, 0), (("up", 2), 2, 0), (("down", 2), 2, 1)):
        b2[key].wait_recv()
        ref = b_part(step, t)
        b3.append(send(ref, ref, partner))

    for copy in totals:
        copy.wait_recv()
    place = lax.broadcasted_iota(jnp.int32, (N_ROW, 8, 128), 0)
    off[...] = within + jnp.sum(jnp.where(place < r, c_b[...], 0), axis=0)

    for copy in a5 + b3:
        copy.wait_recv()
    for copy in started:
        copy.wait_send()


def exchanged(sections, pa, pb, msg):
    bf16, i32 = jnp.bfloat16, jnp.int32
    return pl.pallas_call(
        exchange_kernel,
        out_shape=(
            jax.ShapeDtypeStruct(tiles_of(MOST, 2), bf16),
            jax.ShapeDtypeStruct(tiles_of(16, 2, 4), bf16),
            jax.ShapeDtypeStruct((2, 16, 128), i32),
            jax.ShapeDtypeStruct((2, KT, 128), i32),
            jax.ShapeDtypeStruct((8, 128), i32),
        ),
        in_specs=[SMEM, VMEM, VMEM, VMEM],
        out_specs=(VMEM,) * 5,
        scratch_shapes=[
            pltpu.VMEM(tiles_of(4, 8), bf16),
            pltpu.VMEM(tiles_of(4, 8), bf16),
            pltpu.VMEM(tiles_of(2, 2, 4), bf16),
            pltpu.VMEM(tiles_of(2, 8, 2), bf16),
            pltpu.VMEM(tiles_of(4, 2, 2), bf16),
            pltpu.VMEM(tiles_of(4, 2, 2), bf16),
            pltpu.VMEM(tiles_of(2, 2, 2), bf16),
            pltpu.VMEM(tiles_of(2, 2, 32), bf16),
            pltpu.VMEM(tiles_of(8, 2, 4), bf16),
            pltpu.VMEM(tiles_of(2, 2, 4), bf16),
            pltpu.VMEM(tiles_of(2, 2, 4), bf16),
            pltpu.VMEM(tiles_of(2, 2, 4), bf16),
            pltpu.VMEM(tiles_of(2, 2, 4), bf16),
            pltpu.VMEM((N_COL, 16, 128), i32),
            pltpu.VMEM((N_ROW, 16, 128), i32),
            pltpu.VMEM((N_COL, 8, 128), i32),
            pltpu.VMEM((N_ROW, 8, 128), i32),
            pltpu.VMEM((8, 128), i32),
            pltpu.VMEM((8, 128), i32),
            pltpu.SemaphoreType.DMA((N_SEMS,)),
            pltpu.SemaphoreType.DMA((N_SEMS,)),
        ],
        compiler_params=pltpu.CompilerParams(collective_id=0, has_side_effects=True, vmem_limit_bytes=48 << 20),
        name="exchange",
    )(sections, pa, pb, msg)


def product_kernel(af, bf, afl, bfl, off, packed, places, b_dense, a_rows, staged, masks, sems):
    def unpack_b(n, counts):
        s, k = n // KT, n % KT
        count = jnp.where(k == 0, 0, counts)
        mask = jnp.int32(0)
        for q in range(16):
            flag = bfl[s, k, B_LANE + q]
            tile = bf[count // 4, s, count % 4]
            b_dense[pl.ds(pl.multiple_of(n * TILE, TILE), TILE), q * TILE : (q + 1) * TILE] = jnp.where(
                flag > 0, tile, jnp.zeros_like(tile)
            )
            count = jnp.minimum(count + flag, MOST - 1)
            mask = mask + flag * (1 << q)
        masks[n] = mask
        return count

    lax.fori_loop(0, 2 * KT, unpack_b, jnp.int32(0))

    def row_copy(i):
        rows = pl.ds(pl.multiple_of(i * TILE, TILE), TILE)
        return pltpu.make_async_copy(staged.at[rows], packed.at[rows], sems.at[i])

    def store(slot, tile):
        rows = pl.ds(pl.multiple_of(slot // 16 * TILE, TILE), TILE)
        cols = pl.ds(pl.multiple_of(slot % 16 * TILE, TILE), TILE)
        staged[rows, cols] = tile

    def two_rows(p2, carry):
        count0, count1, slot, done = carry
        counts = [count0, count1]
        row_masks = []
        for pp in range(2):
            mask = jnp.int32(0)
            for s in range(2):
                for k in range(KT):
                    flag = afl[s, p2 * 2 + pp, k]
                    tile = af[counts[s], s]
                    n = s * KT + k
                    a_rows[pp * TILE : (pp + 1) * TILE, n * TILE : (n + 1) * TILE] = jnp.where(
                        flag > 0, tile, jnp.zeros_like(tile)
                    )
                    counts[s] = jnp.minimum(counts[s] + flag, MOST - 1)
                    mask = mask | (masks[n] * flag)
            row_masks.append(mask)
        ahead = jnp.int32(0)
        for q in range(16):
            ahead = ahead + ((row_masks[0] >> q) & 1)
        slots = (slot, slot + ahead)

        def columns(n, slots):
            lhs = a_rows[...]
            rhs = b_dense[:, pl.ds(pl.multiple_of(n * 512, 512), 512)]
            out = jnp.dot(lhs, rhs, preferred_element_type=jnp.float32).astype(jnp.bfloat16)
            slots = list(slots)
            for pp in range(2):
                for q in range(4):
                    bit = (row_masks[pp] >> (n * 4 + q)) & 1

                    @pl.when(bit > 0)
                    def _(pp=pp, q=q, slot=slots[pp]):
                        store(slot, out[pp * TILE : (pp + 1) * TILE, q * TILE : (q + 1) * TILE])

                    slots[pp] = slots[pp] + bit
            return tuple(slots)

        _, slot = lax.fori_loop(0, 4, columns, slots)
        ready = slot // 16

        def out_row(i, _):
            row_copy(i).start()
            return 0

        lax.fori_loop(done, ready, out_row, 0)
        return counts[0], counts[1], slot, ready

    zero = jnp.int32(0)
    _, _, slot, done = lax.fori_loop(0, 8, two_rows, (zero, zero, zero, zero))

    def blank(i, _):
        store(i, jnp.zeros((TILE, TILE), jnp.bfloat16))
        return 0

    lax.fori_loop(slot, 256, blank, 0)

    def out_row(i, _):
        row_copy(i).start()
        return 0

    lax.fori_loop(done, 16, out_row, 0)
    index = lax.broadcasted_iota(jnp.int32, (16, 16), 0) * 16 + lax.broadcasted_iota(jnp.int32, (16, 16), 1)
    places[...] = jnp.where(index < slot, index + off[0:1, 0:1], -1)
    for i in range(16):
        row_copy(i).wait()


def products(af, bf, afl, bfl, off):
    return pl.pallas_call(
        product_kernel,
        out_shape=(
            jax.ShapeDtypeStruct((2048, 2048), jnp.bfloat16),
            jax.ShapeDtypeStruct((16, 16), jnp.int32),
        ),
        in_specs=[VMEM, VMEM, SMEM, SMEM, VMEM],
        out_specs=(ANY, VMEM),
        scratch_shapes=[
            pltpu.VMEM((2048, 2048), jnp.bfloat16),
            pltpu.VMEM((256, 2048), jnp.bfloat16),
            pltpu.VMEM((2048, 2048), jnp.bfloat16),
            pltpu.SMEM((16,), jnp.int32),
            pltpu.SemaphoreType.DMA((16,)),
        ],
        compiler_params=pltpu.CompilerParams(vmem_limit_bytes=48 << 20),
        name="product",
    )(af, bf, afl, bfl, off)


def shards(a_matrix, a_flags, b_matrix, b_flags, sections):
    pa, pb, msg = packed_panels(sections, a_flags, b_flags, a_matrix, b_matrix)
    return products(*exchanged(sections, pa, pb, msg))


def solution(mesh):
    return jax.shard_map(
        shards,
        mesh=mesh,
        in_specs=(P("row", "col"), P("row", "col"), P("row", "col"), P("row", "col"), P()),
        out_specs=(P("row", "col"), P("row", "col")),
        check_vma=False,
    )
```

```python
import jax
import jax.numpy as jnp
from jax import lax
from jax.experimental import pallas as pl
from jax.experimental.pallas import tpu as pltpu
from jax.sharding import PartitionSpec as P

TILE = 128
KT = 8
MOST = 64
N_ROW = 8
N_COL = 16
B_LANE = 16
MESH = pl.DeviceIdType.MESH
VMEM = pl.BlockSpec(memory_space=pltpu.VMEM)
SMEM = pl.BlockSpec(memory_space=pltpu.SMEM)
HBM = pl.BlockSpec(memory_space=pltpu.HBM)


def tiles_of(*lead):
    return (*lead, TILE, TILE)


def pack_kernel(
    sec_h, af_h, bf_h, a_hbm, b_hbm, pa, pb, msg, sec, af, bf, af_v, bf_v, src_a, src_b0, src_b1, sems, small
):
    fetched = [
        pltpu.make_async_copy(src, dst, small.at[n])
        for n, (src, dst) in enumerate(
            ((sec_h, sec), (bf_h, bf), (af_h, af), (af_h, af_v), (bf_h, bf_v))
        )
    ]
    for copy in fetched:
        copy.start()

    def listed(flag_at, count, src):
        def step(i, found):
            src[found] = i
            return found + flag_at(i)

        return lax.fori_loop(0, count, step, jnp.int32(0), unroll=8)

    def copy_of(matrix, row, col, dst, sem):
        return pltpu.make_async_copy(
            matrix.at[pl.ds(pl.multiple_of(row * TILE, TILE), TILE), pl.ds(pl.multiple_of(col * TILE, TILE), TILE)],
            dst,
            sem,
        )

    def start_a():
        found = listed(lambda i: af[i // KT, i % KT], 16 * KT, src_a)

        def go(j, _):
            i = jnp.where(j < found, src_a[j], 0)
            copy_of(a_hbm, i // KT, i % KT, pa.at[j], sems.at[0]).start()
            return 0

        lax.fori_loop(0, MOST, go, 0, unroll=4)

    def start_b(s, src):
        first = (sec[s] % 2) * KT
        found = listed(lambda i: bf[first + i // 16, i % 16], 16 * KT, src)

        def go(j, _):
            i = jnp.where(j < found, src[j], 0)
            copy_of(b_hbm, first + i // 16, i % 16, pb.at[s, j], sems.at[1 + s]).start()
            return 0

        lax.fori_loop(0, MOST, go, 0, unroll=4)

    for copy in fetched[:3]:
        copy.wait()
    start_b(0, src_b0)
    start_b(1, src_b1)
    start_a()
    for copy in fetched[3:]:
        copy.wait()
    msg[...] = jnp.zeros_like(msg)
    msg[:, 0:KT] = af_v[...]
    msg[:, B_LANE : B_LANE + 16] = bf_v[...]
    pltpu.make_async_copy(pb.at[0], pb.at[0], sems.at[1]).wait()
    pltpu.make_async_copy(pb.at[1], pb.at[1], sems.at[2]).wait()
    pltpu.make_async_copy(pa, pa, sems.at[0]).wait()


def packed_panels(sections, a_flags, b_flags, a_matrix, b_matrix):
    return pl.pallas_call(
        pack_kernel,
        out_shape=(
            pltpu.VMEM(tiles_of(MOST), jnp.bfloat16),
            pltpu.VMEM(tiles_of(2, MOST), jnp.bfloat16),
            pltpu.VMEM((16, 128), jnp.int32),
        ),
        in_specs=[HBM] * 5,
        out_specs=(VMEM, VMEM, VMEM),
        scratch_shapes=[
            pltpu.SMEM((2,), jnp.int32),
            pltpu.SMEM((16, KT), jnp.int32),
            pltpu.SMEM((16, 16), jnp.int32),
            pltpu.VMEM((16, KT), jnp.int32),
            pltpu.VMEM((16, 16), jnp.int32),
            pltpu.SMEM((136,), jnp.int32),
            pltpu.SMEM((136,), jnp.int32),
            pltpu.SMEM((136,), jnp.int32),
            pltpu.SemaphoreType.DMA((3,)),
            pltpu.SemaphoreType.DMA((6,)),
        ],
        compiler_params=pltpu.CompilerParams(vmem_limit_bytes=16 << 20),
        name="pack",
    )(*(pltpu.with_memory_space_constraint(v, pltpu.HBM) for v in (sections, a_flags, b_flags, a_matrix, b_matrix)))


N_SEMS = 160


def exchange_kernel(
    sec, pa, pb, msg,
    af, bf, afl, bfl, off,
    cand_0, cand_1, trans, pick, cand2_0, cand2_1, trans2,
    x_buf, y_buf, z_tr, z_dir, z_mg, z_send,
    f_a, f_b, c_a, c_b, cnt, tot,
    send_sems, recv_sems,
):
    cand, cand2 = (cand_0, cand_1), (cand2_0, cand2_1)
    r, c = lax.axis_index("row"), lax.axis_index("col")
    z, core = r // 2, r % 2
    y, x = c // 4, c % 4
    pos = {"x": x, "y": y, "z": z}

    def at(dim, step):
        where = dict(pos)
        where[dim] = (pos[dim] + step) % 4
        return (where["z"] * 2 + core, where["y"] * 4 + where["x"])

    partner = (z * 2 + 1 - core, c)
    col_peers = [(r, (c + d) % N_COL) for d in range(1, N_COL)]
    row_peers = [((r + d) % N_ROW, c) for d in range(1, N_ROW)]

    barrier = pltpu.get_barrier_semaphore()
    for peer in col_peers + row_peers:
        pl.semaphore_signal(barrier, inc=1, device_id=peer, device_id_type=MESH)
    pl.semaphore_wait(barrier, len(col_peers) + len(row_peers))

    started = []

    def send(src, dst, peer):
        n = len(started)
        copy = pltpu.make_async_remote_copy(
            src_ref=src, dst_ref=dst, send_sem=send_sems.at[n], recv_sem=recv_sems.at[n],
            device_id=peer, device_id_type=MESH,
        )
        copy.start()
        started.append(copy)
        return copy

    sec_v = [sec[0], sec[1]]
    root = [{"x": lax.rem(v, 4), "y": lax.div(v, 4), "z": lax.div(v, 4)} for v in sec_v]
    root_core = [lax.rem(lax.div(v, 2), 2) for v in sec_v]

    flags_row = [send(msg, f_a.at[c], peer) for peer in col_peers]
    flags_col = [send(msg, f_b.at[r], peer) for peer in row_peers]

    axes = (("x", "y"), ("y", "x"))
    a1 = []
    for h in range(2):
        d, p = axes[h][0], pos[axes[h][0]]
        far = h * 32 + ((p + 2) % 4) * 8
        a1.append([
            send(pa.at[pl.ds(far, 4)], trans.at[h, 0], at(d, 1)),
            send(pa.at[pl.ds(far + 4, 4)], trans.at[h, 1], at(d, 3)),
        ])
    b0 = [send(pb.at[s, pl.ds((1 - core) * 32, 32)], x_buf.at[s, core], partner) for s in range(2)]
    for h in range(2):
        d, p = axes[h][0], pos[axes[h][0]]
        a1[h] += [
            send(pa.at[pl.ds(h * 32 + ((p + 1) % 4) * 8, 8)], cand[h].at[p], at(d, 1)),
            send(pa.at[pl.ds(h * 32 + ((p + 3) % 4) * 8, 8)], cand[h].at[p], at(d, 3)),
        ]
    f_a[c] = msg[...]
    f_b[r] = msg[...]
    for s in range(2):
        x_buf[s, core] = pb[s, pl.ds(core * 32, 32)]
    for h in range(2):
        p = pos[axes[h][0]]
        cand[h][p] = pa[pl.ds(h * 32 + p * 8, 8)]

    for copy in flags_row + flags_col:
        copy.wait_recv()
    inter = jnp.zeros((16, 128), jnp.int32)
    for s in range(2):
        a_own = f_a[sec_v[s]]
        b_pair = f_b[lax.div(sec_v[s], 2)]
        b_own = jnp.where(lax.rem(sec_v[s], 2) == 0, b_pair[0:KT], b_pair[KT:])
        afl[s] = a_own
        bfl[s] = b_own
        for k in range(KT):
            inter = inter + a_own[:, k : k + 1] * b_own[k : k + 1, :]
    lane = lax.broadcasted_iota(jnp.int32, (16, 128), 1)
    held = (inter > 0) & (lane >= B_LANE) & (lane < B_LANE + 16)
    filled = jnp.sum(jnp.where(held, 1, 0), axis=(0, 1), keepdims=True)
    cnt[...] = jnp.broadcast_to(filled, (8, 128))
    counts = [send(cnt, c_a.at[c], peer) for peer in col_peers]
    c_a[c] = cnt[...]

    for copy in b0:
        copy.wait_recv()
    for s in range(2):
        for i in range(8):
            y_buf[i, s] = x_buf[s, root_core[s], i * 4 : i * 4 + 4]
    w = z
    b1 = [
        send(y_buf.at[((w + 2) % 4) * 2], z_tr.at[0], at("z", 1)),
        send(y_buf.at[((w + 2) % 4) * 2 + 1], z_tr.at[1], at("z", 3)),
        send(y_buf.at[((w + 1) % 4) * 2 + 1], z_dir.at[1], at("z", 1)),
        send(y_buf.at[((w + 3) % 4) * 2], z_dir.at[0], at("z", 3)),
    ]

    for h in range(2):
        d, p = axes[h][0], pos[axes[h][0]]
        a1[h][0].wait_recv()
        a1[h].append(send(trans.at[h, 0], cand[h].at[(p + 3) % 4, pl.ds(0, 4)], at(d, 1)))
        a1[h][1].wait_recv()
        a1[h].append(send(trans.at[h, 1], cand[h].at[(p + 1) % 4, pl.ds(4, 4)], at(d, 3)))

    for copy in counts:
        copy.wait_recv()
    place = lax.broadcasted_iota(jnp.int32, (N_COL, 8, 128), 0)
    all_counts = c_a[...]
    within = jnp.sum(jnp.where(place < c, all_counts, 0), axis=0)
    tot[...] = jnp.sum(all_counts, axis=0)
    totals = [send(tot, c_b.at[r], peer) for peer in row_peers]
    c_b[r] = tot[...]

    a2 = []
    for h in range(2):
        for n in (2, 3, 4, 5):
            a1[h][n].wait_recv()
        d, q = axes[h][1], pos[axes[h][1]]
        for s in range(2):
            for j in range(8):
                pick[h, j, s] = cand[h][root[s][axes[h][0]], j]
        far = ((q + 2) % 4) * 2
        a2.append([
            send(pick.at[h, far], trans2.at[h, 0], at(d, 1)),
            send(pick.at[h, far + 1], trans2.at[h, 1], at(d, 3)),
            send(pick.at[h, pl.ds(((q + 1) % 4) * 2, 2)], cand2[h].at[q], at(d, 1)),
            send(pick.at[h, pl.ds(((q + 3) % 4) * 2, 2)], cand2[h].at[q], at(d, 3)),
        ])
        cand2[h][q] = pick[h, pl.ds(q * 2, 2)]

    def z_merged(t, own_at):
        for s in range(2):
            here = root[s]["z"] == w
            z_send[t, s] = jnp.where(here, y_buf[own_at, s], z_tr[t, s])

    b1[0].wait_recv()
    z_merged(0, ((w + 1) % 4) * 2)
    b1.append(send(z_send.at[0], z_mg.at[0], at("z", 1)))
    b1[1].wait_recv()
    z_merged(1, ((w + 3) % 4) * 2 + 1)
    b1.append(send(z_send.at[1], z_mg.at[1], at("z", 3)))

    for h in range(2):
        d, q = axes[h][1], pos[axes[h][1]]
        a2[h][0].wait_recv()
        a2[h].append(send(trans2.at[h, 0], cand2[h].at[(q + 3) % 4, 0], at(d, 1)))
        a2[h][1].wait_recv()
        a2[h].append(send(trans2.at[h, 1], cand2[h].at[(q + 1) % 4, 1], at(d, 3)))

    def a_slot(h, p, q):
        return h * 32 + p * 8 + q * 2

    a3 = []
    for h in range(2):
        for n in (2, 3, 4, 5):
            a2[h][n].wait_recv()
        p, (d, q) = pos[axes[h][0]], (axes[h][1], pos[axes[h][1]])
        own = a_slot(h, p, q)
        for s in range(2):
            for t in range(2):
                af[own + t, s] = cand2[h][root[s][d], t, s]
        block = af.at[pl.ds(own, 2)]
        a3.append([send(block, block, at(d, 1)), send(block, block, at(d, 3))])

    a4 = []

    def a_out(h, e):
        d, p = axes[h][0], pos[axes[h][0]]
        q = (pos[axes[h][1]] - e) % 4
        block = af.at[pl.ds(a_slot(h, p, q), 2)]
        a4.append((h, q, send(block, block, at(d, 1)), send(block, block, at(d, 3))))

    for h in range(2):
        a_out(h, 0)
    for h in range(2):
        d, p, q = axes[h][1], pos[axes[h][0]], pos[axes[h][1]]
        a3[h][0].wait_recv()
        part = af.at[a_slot(h, p, (q + 3) % 4)]
        a3[h].append(send(part, part, at(d, 1)))
        a3[h][1].wait_recv()
        part = af.at[a_slot(h, p, (q + 1) % 4) + 1]
        a3[h].append(send(part, part, at(d, 3)))
    for e in (1, 3):
        for h in range(2):
            a_out(h, e)

    b1[4].wait_recv()
    b1[5].wait_recv()
    b1[2].wait_recv()
    b1[3].wait_recv()
    mine = core * 8 + w * 2
    for t in range(2):
        for s in range(2):
            ahead = lax.rem(root[s]["z"] - w + 4, 4)
            near = 1 if t == 0 else 3
            got = jnp.where(ahead == near, z_dir[t, s], z_mg[t, s])
            bf[mine + t, s] = jnp.where(ahead == 0, y_buf[w * 2 + t, s], got)

    b2 = {}
    b3 = []

    def b_part(step, t):
        return bf.at[core * 8 + ((w + step) % 4) * 2 + t]

    for t in range(2):
        ref = b_part(0, t)
        b2["up", t] = send(ref, ref, at("z", 1))
        ref = b_part(0, 1 - t)
        b2["down", 1 - t] = send(ref, ref, at("z", 3))
    for t in range(2):
        ref = b_part(0, t)
        b3.append(send(ref, ref, partner))

    for h in range(2):
        a3[h][2].wait_recv()
        a3[h][3].wait_recv()
        a_out(h, 2)

    a5 = []

    def a_forward(n):
        h, q, up, down = a4[n]
        d, p = axes[h][0], pos[axes[h][0]]
        up.wait_recv()
        part = af.at[a_slot(h, (p + 3) % 4, q)]
        a5.append(send(part, part, at(d, 1)))
        down.wait_recv()
        part = af.at[a_slot(h, (p + 1) % 4, q) + 1]
        a5.append(send(part, part, at(d, 3)))

    for n in range(4):
        a_forward(n)
    b2["up", 0].wait_recv()
    ref = b_part(3, 0)
    b2["up", 2] = send(ref, ref, at("z", 1))
    b3.append(send(ref, ref, partner))
    b2["down", 1].wait_recv()
    ref = b_part(1, 1)
    b2["down", 2] = send(ref, ref, at("z", 3))
    b3.append(send(ref, ref, partner))
    for n in range(4, 8):
        a_forward(n)
    for key, step, t in ((("up", 1), 3, 1), (("down", 0), 1, 0), (("up", 2), 2, 0), (("down", 2), 2, 1)):
        b2[key].wait_recv()
        ref = b_part(step, t)
        b3.append(send(ref, ref, partner))

    for copy in totals:
        copy.wait_recv()
    place = lax.broadcasted_iota(jnp.int32, (N_ROW, 8, 128), 0)
    off[...] = within + jnp.sum(jnp.where(place < r, c_b[...], 0), axis=0)

    for copy in a5 + b3:
        copy.wait_recv()
    for copy in started:
        copy.wait_send()


def exchanged(sections, pa, pb, msg):
    bf16, i32 = jnp.bfloat16, jnp.int32
    return pl.pallas_call(
        exchange_kernel,
        out_shape=(
            pltpu.VMEM(tiles_of(MOST, 2), bf16),
            pltpu.VMEM(tiles_of(16, 2, 4), bf16),
            pltpu.VMEM((2, 16, 128), i32),
            pltpu.VMEM((2, KT, 128), i32),
            pltpu.VMEM((8, 128), i32),
        ),
        in_specs=[SMEM, VMEM, VMEM, VMEM],
        out_specs=(VMEM,) * 5,
        scratch_shapes=[
            pltpu.VMEM(tiles_of(4, 8), bf16),
            pltpu.VMEM(tiles_of(4, 8), bf16),
            pltpu.VMEM(tiles_of(2, 2, 4), bf16),
            pltpu.VMEM(tiles_of(2, 8, 2), bf16),
            pltpu.VMEM(tiles_of(4, 2, 2), bf16),
            pltpu.VMEM(tiles_of(4, 2, 2), bf16),
            pltpu.VMEM(tiles_of(2, 2, 2), bf16),
            pltpu.VMEM(tiles_of(2, 2, 32), bf16),
            pltpu.VMEM(tiles_of(8, 2, 4), bf16),
            pltpu.VMEM(tiles_of(2, 2, 4), bf16),
            pltpu.VMEM(tiles_of(2, 2, 4), bf16),
            pltpu.VMEM(tiles_of(2, 2, 4), bf16),
            pltpu.VMEM(tiles_of(2, 2, 4), bf16),
            pltpu.VMEM((N_COL, 16, 128), i32),
            pltpu.VMEM((N_ROW, 16, 128), i32),
            pltpu.VMEM((N_COL, 8, 128), i32),
            pltpu.VMEM((N_ROW, 8, 128), i32),
            pltpu.VMEM((8, 128), i32),
            pltpu.VMEM((8, 128), i32),
            pltpu.SemaphoreType.DMA((N_SEMS,)),
            pltpu.SemaphoreType.DMA((N_SEMS,)),
        ],
        compiler_params=pltpu.CompilerParams(collective_id=0, has_side_effects=True, vmem_limit_bytes=30 << 20),
        name="exchange",
    )(sections, pa, pb, msg)


def product_kernel(af, bf, afl, bfl, off, packed, places, b_dense, a_rows, staged, masks, sems):
    def unpack_b(n, counts):
        s, k = n // KT, n % KT
        count = jnp.where(k == 0, 0, counts)
        mask = jnp.int32(0)
        for q in range(16):
            flag = bfl[s, k, B_LANE + q]
            tile = bf[count // 4, s, count % 4]
            b_dense[pl.ds(pl.multiple_of(n * TILE, TILE), TILE), q * TILE : (q + 1) * TILE] = jnp.where(
                flag > 0, tile, jnp.zeros_like(tile)
            )
            count = jnp.minimum(count + flag, MOST - 1)
            mask = mask + flag * (1 << q)
        masks[n] = mask
        return count

    lax.fori_loop(0, 2 * KT, unpack_b, jnp.int32(0))

    def row_copy(i):
        rows = pl.ds(pl.multiple_of(i * TILE, TILE), TILE)
        return pltpu.make_async_copy(staged.at[rows], packed.at[rows], sems.at[i])

    def store(slot, tile):
        rows = pl.ds(pl.multiple_of(slot // 16 * TILE, TILE), TILE)
        cols = pl.ds(pl.multiple_of(slot % 16 * TILE, TILE), TILE)
        staged[rows, cols] = tile

    def two_rows(p2, carry):
        count0, count1, slot, done = carry
        counts = [count0, count1]
        row_masks = []
        for pp in range(2):
            mask = jnp.int32(0)
            for s in range(2):
                for k in range(KT):
                    flag = afl[s, p2 * 2 + pp, k]
                    tile = af[counts[s], s]
                    n = s * KT + k
                    a_rows[pp * TILE : (pp + 1) * TILE, n * TILE : (n + 1) * TILE] = jnp.where(
                        flag > 0, tile, jnp.zeros_like(tile)
                    )
                    counts[s] = jnp.minimum(counts[s] + flag, MOST - 1)
                    mask = mask | (masks[n] * flag)
            row_masks.append(mask)
        ahead = jnp.int32(0)
        for q in range(16):
            ahead = ahead + ((row_masks[0] >> q) & 1)
        slots = (slot, slot + ahead)

        def columns(n, slots):
            lhs = a_rows[...]
            rhs = b_dense[:, pl.ds(pl.multiple_of(n * 512, 512), 512)]
            out = jnp.dot(lhs, rhs, preferred_element_type=jnp.float32).astype(jnp.bfloat16)
            slots = list(slots)
            for pp in range(2):
                for q in range(4):
                    bit = (row_masks[pp] >> (n * 4 + q)) & 1

                    @pl.when(bit > 0)
                    def _(pp=pp, q=q, slot=slots[pp]):
                        store(slot, out[pp * TILE : (pp + 1) * TILE, q * TILE : (q + 1) * TILE])

                    slots[pp] = slots[pp] + bit
            return tuple(slots)

        _, slot = lax.fori_loop(0, 4, columns, slots)
        ready = slot // 16

        def out_row(i, _):
            row_copy(i).start()
            return 0

        lax.fori_loop(done, ready, out_row, 0)
        return counts[0], counts[1], slot, ready

    zero = jnp.int32(0)
    _, _, slot, done = lax.fori_loop(0, 8, two_rows, (zero, zero, zero, zero))

    def blank(i, _):
        store(i, jnp.zeros((TILE, TILE), jnp.bfloat16))
        return 0

    lax.fori_loop(slot, 256, blank, 0)

    def out_row(i, _):
        row_copy(i).start()
        return 0

    lax.fori_loop(done, 16, out_row, 0)
    index = lax.broadcasted_iota(jnp.int32, (16, 16), 0) * 16 + lax.broadcasted_iota(jnp.int32, (16, 16), 1)
    places[...] = jnp.where(index < slot, index + off[0:1, 0:1], -1)
    for i in range(16):
        row_copy(i).wait()


def products(af, bf, afl, bfl, off):
    return pl.pallas_call(
        product_kernel,
        out_shape=(
            jax.ShapeDtypeStruct((2048, 2048), jnp.bfloat16),
            jax.ShapeDtypeStruct((16, 16), jnp.int32),
        ),
        in_specs=[VMEM, VMEM, SMEM, SMEM, VMEM],
        out_specs=(HBM, VMEM),
        scratch_shapes=[
            pltpu.VMEM((2048, 2048), jnp.bfloat16),
            pltpu.VMEM((256, 2048), jnp.bfloat16),
            pltpu.VMEM((2048, 2048), jnp.bfloat16),
            pltpu.SMEM((16,), jnp.int32),
            pltpu.SemaphoreType.DMA((16,)),
        ],
        compiler_params=pltpu.CompilerParams(vmem_limit_bytes=36 << 20),
        name="product",
    )(af, bf, afl, bfl, off)


def shards(a_matrix, a_flags, b_matrix, b_flags, sections):
    pa, pb, msg = packed_panels(sections, a_flags, b_flags, a_matrix, b_matrix)
    return products(*exchanged(sections, pa, pb, msg))


def solution(mesh):
    return jax.shard_map(
        shards,
        mesh=mesh,
        in_specs=(P("row", "col"), P("row", "col"), P("row", "col"), P("row", "col"), P()),
        out_specs=(P("row", "col"), P("row", "col")),
        check_vma=False,
    )
```
